32 devices in a mesh: row: 4 (over z), col: 8 (over y, x, core).
Axes of the slice: x: 2, y: 2, z: 4, core: 2. Of those that a mesh axis runs over, the one named last changes fastest.
Arguments:
- minus_gradient: float32 [6, 16384], P(None, ('row', 'col')), may hold values from -10 to 10
- diag_blocks: float32 [36, 16384], P(None, ('row', 'col')), may hold values from -1000 to 1000, as said below
- hess_blocks: float32 [4, 8, 36, 4096], P('row', 'col'), may hold values from -40 to 40, as said below
- block_rows: int32 [4, 8, 4096], P('row', 'col'), may hold values from 0 to 2047
- block_cols: int32 [4, 8, 4096], P('row', 'col'), may hold values from 0 to 4095
- block_counts: int32 [4, 8], P('row', 'col'), may hold values from 0 to 4096, as said below
Outputs:
- pose_update: float32 [6, 16384], P(None, ('row', 'col'))
- residual: float32 [6, 16384], P(None, ('row', 'col'))
The draws below stay inside these ranges and needn't reach their ends.
Inputs may be any that keep to these rules, and one draw needn't show every extreme that they name: `hess_blocks`: the live blocks of all tiles together with diag_blocks form a symmetric positive definite matrix; no live block lies on the diagonal; the slots after the live ones hold arbitrary entries. `diag_blocks`: each 6x6 block is symmetric positive definite. The live slots of a tile are its first block_counts slots.
All inputs are finite; a program needn't handle non-finite values.
Results may differ from the reference program's by a relative error of at most 0.0003.
Values sent between devices are 32-bit elements; how exact they have to be, the bound alone decides.
No kernel may reach another device: no remote copies, remote signals or barrier semaphores. Data moves between devices by JAX's collectives and lax.ppermute only.
A program may use at most 64 MiB of HBM per device.

```python
import jax
import jax.numpy as jnp
from jax import lax

POSE_DEV = 512
ITERS = 3
SLOTS = 4096
LOOPS = 16384
N_ROW = 4
N_COL = 8


damping = 0.5


def skewed_index(key, count, length):
    first_key, second_key = jax.random.split(key)
    factor_one = jax.random.randint(first_key, (count,), 0, length)
    factor_two = jax.random.randint(second_key, (count,), 1, length + 1)
    return factor_one * factor_two // length


def tile_ranks(tile_key):
    ordering = jnp.argsort(tile_key, stable=True)
    ordered = tile_key[ordering]
    first_pos = jnp.searchsorted(ordered, ordered, side='left').astype(jnp.int32)
    ranked = jnp.arange(tile_key.shape[0], dtype=jnp.int32) - first_pos
    return jnp.zeros_like(tile_key).at[ordering].set(ranked)


def build_graph(key):
    pose_count = POSE_DEV * N_ROW * N_COL
    group_size = POSE_DEV * N_COL
    devices = N_ROW * N_COL
    subkeys = jax.random.split(key, 14)
    col_order = jax.random.permutation(subkeys[0], N_COL).astype(jnp.int32)
    row_order = jax.random.permutation(subkeys[1], N_ROW).astype(jnp.int32)
    col_source = col_order[skewed_index(subkeys[2], LOOPS, N_COL)]
    row_source = jax.random.randint(subkeys[3], (LOOPS,), 0, N_ROW)
    row_target = row_order[skewed_index(subkeys[4], LOOPS, N_ROW)]
    col_target = jax.random.randint(subkeys[5], (LOOPS,), 0, N_COL)
    pose_source = (row_source * N_COL + col_source) * POSE_DEV + jax.random.randint(subkeys[6], (LOOPS,), 0, POSE_DEV)
    pose_target = (row_target * N_COL + col_target) * POSE_DEV + jax.random.randint(subkeys[7], (LOOPS,), 0, POSE_DEV)
    pose_target = jnp.where(pose_target == pose_source, (pose_target + 1) % pose_count, pose_target)
    chain_start = jnp.arange(pose_count - 1, dtype=jnp.int32)
    sources = jnp.concatenate([chain_start, pose_source.astype(jnp.int32)])
    targets = jnp.concatenate([chain_start + 1, pose_target.astype(jnp.int32)])
    edge_count = pose_count - 1 + LOOPS
    jacobian_left = jax.random.normal(subkeys[9], (edge_count, 6, 6)) * 6.0 ** (-0.5)
    jacobian_right = jax.random.normal(subkeys[10], (edge_count, 6, 6)) * 6.0 ** (-0.5)
    off_forward = jnp.einsum('eki,ekj->eij', jacobian_left, jacobian_right).reshape(edge_count, 36)
    off_backward = jnp.einsum('eki,ekj->eij', jacobian_right, jacobian_left).reshape(edge_count, 36)
    all_rows = jnp.concatenate([sources, targets])
    all_cols = jnp.concatenate([targets, sources])
    values = jnp.concatenate([off_forward, off_backward])
    seg_rows = all_rows // POSE_DEV
    seg_cols = all_cols // POSE_DEV
    tile_row = seg_cols // N_COL
    tile_col = seg_rows % N_COL
    tile_ids = tile_row * N_COL + tile_col
    local_row = seg_rows // N_COL * POSE_DEV + all_rows % POSE_DEV
    local_col = all_cols - tile_row * group_size
    first_rank = tile_ranks(tile_ids)
    overflow = first_rank >= SLOTS
    keep_edge = jnp.logical_not(jnp.logical_or(overflow[:edge_count], overflow[edge_count:]))
    keep_all = jnp.concatenate([keep_edge, keep_edge])
    second_rank = tile_ranks(jnp.where(keep_all, tile_ids, devices))
    target_slot = jnp.where(keep_all, tile_ids * SLOTS + second_rank, devices * SLOTS)
    pad_rows = jax.random.randint(subkeys[11], (devices * SLOTS,), 0, N_ROW * POSE_DEV)
    pad_cols = jax.random.randint(subkeys[12], (devices * SLOTS,), 0, group_size)
    rows_out = pad_rows.at[target_slot].set(local_row, mode='drop').reshape(N_ROW, N_COL, SLOTS)
    cols_out = pad_cols.at[target_slot].set(local_col, mode='drop').reshape(N_ROW, N_COL, SLOTS)
    pad_values = jnp.clip(jax.random.normal(subkeys[13], (devices * SLOTS, 36)), -3.0, 3.0) * 0.5
    hess_out = pad_values.at[target_slot].set(values, mode='drop').reshape(N_ROW, N_COL, SLOTS, 36)
    hess_out = jnp.transpose(hess_out, (0, 1, 3, 2))
    counts_out = jax.ops.segment_sum(keep_all.astype(jnp.int32), tile_ids, num_segments=devices).reshape(N_ROW, N_COL)
    keep_float = keep_edge.astype(jnp.float32)[:, None]
    own_left = jnp.einsum('eki,ekj->eij', jacobian_left, jacobian_left).reshape(edge_count, 36) * keep_float
    own_right = jnp.einsum('eki,ekj->eij', jacobian_right, jacobian_right).reshape(edge_count, 36) * keep_float
    diagonal = jax.ops.segment_sum(own_left, sources, num_segments=pose_count)
    diagonal = diagonal + jax.ops.segment_sum(own_right, targets, num_segments=pose_count)
    diagonal = diagonal + damping * jnp.eye(6, dtype=jnp.float32).reshape(1, 36)
    return (hess_out, rows_out, cols_out, counts_out, jnp.transpose(diagonal))


def draw_hess_blocks(key, part):
    return build_graph(jax.random.fold_in(key, 11))[0]


def draw_block_rows(key, part):
    return build_graph(jax.random.fold_in(key, 11))[1]


def draw_block_cols(key, part):
    return build_graph(jax.random.fold_in(key, 11))[2]


def draw_block_counts(key, part):
    return build_graph(jax.random.fold_in(key, 11))[3]


def draw_diag_blocks(key, part):
    return build_graph(jax.random.fold_in(key, 11))[4]


def draw_minus_gradient(key, part):
    pose_count = POSE_DEV * N_ROW * N_COL
    scale_ramp = 0.5 + jnp.arange(pose_count, dtype=jnp.float32) / pose_count
    values = jnp.clip(jax.random.normal(key, (6, pose_count)), -6.0, 6.0) * scale_ramp
    return values


def setup_inputs(seed: int = 0) -> dict:
    keys = jax.random.split(jax.random.key(seed), 7)
    return {
        "minus_gradient": draw_minus_gradient(jax.random.fold_in(keys[6], 71), 0),
        "diag_blocks": draw_diag_blocks(jax.random.fold_in(keys[6], 71), 0),
        "hess_blocks": draw_hess_blocks(jax.random.fold_in(keys[6], 71), 0),
        "block_rows": draw_block_rows(jax.random.fold_in(keys[6], 71), 0),
        "block_cols": draw_block_cols(jax.random.fold_in(keys[6], 71), 0),
        "block_counts": draw_block_counts(jax.random.fold_in(keys[6], 71), 0),
    }


def factor_blocks(blocks):
    lower_part = {}
    reciprocals = []
    for j in range(6):
        pivot_value = blocks[7 * j]
        for k in range(j):
            pivot_value = pivot_value - lower_part[j, k] * lower_part[j, k]
        reciprocal = 1.0 / jnp.sqrt(pivot_value)
        reciprocals.append(reciprocal)
        for i in range(j + 1, 6):
            entry_value = blocks[6 * i + j]
            for k in range(j):
                entry_value = entry_value - lower_part[i, k] * lower_part[j, k]
            lower_part[i, j] = entry_value * reciprocal
    return (lower_part, reciprocals)

def apply_inverse(lower_part, reciprocals, vector):
    forward = []
    for i in range(6):
        running = vector[i]
        for k in range(i):
            running = running - lower_part[i, k] * forward[k]
        forward.append(running * reciprocals[i])
    backward = [None] * 6
    for i in range(5, -1, -1):
        running = forward[i]
        for k in range(i + 1, 6):
            running = running - lower_part[k, i] * backward[k]
        backward[i] = running * reciprocals[i]
    return jnp.stack(backward)

def diagonal_term(diag_blocks, vector):
    return lax.optimization_barrier(jnp.sum(diag_blocks.reshape(6, 6, -1) * vector[None], axis=1))

def apply_hessian(vector, diag_blocks, hess_blocks, block_rows, block_cols, block_counts):
    group_size = POSE_DEV * N_COL
    slot_ids = jnp.arange(SLOTS, dtype=jnp.int32)
    col_ids = jnp.arange(N_COL, dtype=jnp.int32)[:, None]

    def one_row(summed, r):
        blocks = hess_blocks[r].reshape(N_COL, 6, 6, SLOTS)
        local_rows = block_rows[r]
        global_rows = (local_rows // POSE_DEV * N_COL + col_ids) * POSE_DEV + local_rows % POSE_DEV
        global_cols = r * group_size + block_cols[r]
        live_mask = slot_ids[None, :] < block_counts[r][:, None]
        picked = jnp.take(vector, global_cols.reshape(-1), axis=1).reshape(6, N_COL, SLOTS)
        product = lax.optimization_barrier(jnp.sum(blocks * jnp.transpose(picked, (1, 0, 2))[:, None], axis=2))
        product = jnp.where(live_mask[:, None, :], product, 0.0)
        summed = summed.at[:, global_rows.reshape(-1)].add(jnp.transpose(product, (1, 0, 2)).reshape(6, -1))
        return (summed, None)
    summed, unused = lax.scan(one_row, jnp.zeros_like(vector), jnp.arange(N_ROW, dtype=jnp.int32))
    return summed + diagonal_term(diag_blocks, vector)

def reference(minus_gradient, diag_blocks, hess_blocks, block_rows, block_cols, block_counts):
    lower_part, reciprocals = factor_blocks(diag_blocks)

    def hessian(vector):
        return apply_hessian(vector, diag_blocks, hess_blocks, block_rows, block_cols, block_counts)
    solution = jnp.zeros_like(minus_gradient)
    residual = minus_gradient
    precond = apply_inverse(lower_part, reciprocals, residual)
    direction = precond
    rho_now = jnp.sum(residual * precond)
    for k in range(ITERS):
        hess_image = hessian(direction)
        step_size = rho_now / jnp.sum(direction * hess_image)
        solution = solution + step_size * direction
        residual = residual - step_size * hess_image
        if k + 1 < ITERS:
            precond = apply_inverse(lower_part, reciprocals, residual)
            rho_next = jnp.sum(residual * precond)
            direction = precond + rho_next / rho_now * direction
            rho_now = rho_next
    return (solution, residual)
```

```python
import jax
import jax.numpy as jnp
from jax import lax
from jax.experimental import pallas as pl
from jax.experimental.pallas import tpu as pltpu
from jax.sharding import PartitionSpec as P

ITERS = 3
LANES = 128


def factor_blocks(blocks):
    lower_part = {}
    reciprocals = []
    for j in range(6):
        pivot_value = blocks[7 * j]
        for k in range(j):
            pivot_value = pivot_value - lower_part[j, k] * lower_part[j, k]
        reciprocal = 1.0 / jnp.sqrt(pivot_value)
        reciprocals.append(reciprocal)
        for i in range(j + 1, 6):
            entry_value = blocks[6 * i + j]
            for k in range(j):
                entry_value = entry_value - lower_part[i, k] * lower_part[j, k]
            lower_part[i, j] = entry_value * reciprocal
    return (lower_part, reciprocals)


def apply_inverse(lower_part, reciprocals, vector):
    forward = []
    for i in range(6):
        running = vector[i]
        for k in range(i):
            running = running - lower_part[i, k] * forward[k]
        forward.append(running * reciprocals[i])
    backward = [None] * 6
    for i in range(5, -1, -1):
        running = forward[i]
        for k in range(i + 1, 6):
            running = running - lower_part[k, i] * backward[k]
        backward[i] = running * reciprocals[i]
    return backward


def split_three(value):
    high = value.astype(jnp.bfloat16)
    rest = value - high.astype(jnp.float32)
    middle = rest.astype(jnp.bfloat16)
    low = (rest - middle.astype(jnp.float32)).astype(jnp.bfloat16)
    return high, middle, low


def exact_dot(left, onehot, dims):
    parts = [
        lax.dot_general(piece, onehot, (dims, ((), ())), preferred_element_type=jnp.float32)
        for piece in split_three(left)
    ]
    return parts[2] + parts[1] + parts[0]


def tile_kernel(count_ref, table_ref, cols_ref, rows_ref, blocks_ref, out_ref, *, chunk):
    high_in = table_ref.shape[0] // 6
    high_out = out_ref.shape[0] // 6
    slots = cols_ref.shape[1]
    live = count_ref[0, 0]
    table = table_ref[...]
    out_ref[...] = jnp.zeros_like(out_ref)

    def one_chunk(start):
        cols = cols_ref[:, pl.ds(start, chunk)]
        rows = rows_ref[:, pl.ds(start, chunk)]
        lane_ids = lax.broadcasted_iota(jnp.int32, (LANES, chunk), 0)
        low_in = jnp.where(lane_ids == cols % LANES, 1.0, 0.0).astype(jnp.bfloat16)
        spread = exact_dot(table, low_in, ((1,), (0,)))
        pick = lax.broadcasted_iota(jnp.int32, (high_in, chunk), 0) == cols // LANES
        picked = [
            jnp.sum(
                jnp.where(pick, spread[b * high_in : (b + 1) * high_in], 0.0),
                axis=0,
                keepdims=True,
            )
            for b in range(6)
        ]
        is_live = lax.broadcasted_iota(jnp.int32, (1, chunk), 1) + start < live
        place = lax.broadcasted_iota(jnp.int32, (high_out, chunk), 0) == rows // LANES
        terms = []
        for a in range(6):
            term = blocks_ref[6 * a : 6 * a + 1, pl.ds(start, chunk)] * picked[0]
            for b in range(1, 6):
                entry = blocks_ref[6 * a + b : 6 * a + b + 1, pl.ds(start, chunk)]
                term = term + entry * picked[b]
            term = jnp.where(is_live, term, 0.0)
            terms.append(jnp.where(place, term, 0.0))
        low_out = jnp.where(lane_ids == rows % LANES, 1.0, 0.0).astype(jnp.bfloat16)
        out_ref[...] += exact_dot(jnp.concatenate(terms, axis=0), low_out, ((1,), (1,)))

    for turn in range(slots // chunk):
        @pl.when(turn * chunk < live)
        def _():
            one_chunk(turn * chunk)


def tile_product(count, table, cols, rows, blocks, high_out):
    slots = cols.shape[1]
    chunk = min(512, slots)
    vmem = pl.BlockSpec(memory_space=pltpu.VMEM)
    return pl.pallas_call(
        lambda *refs: tile_kernel(*refs, chunk=chunk),
        out_shape=jax.ShapeDtypeStruct((6 * high_out, LANES), jnp.float32),
        in_specs=[pl.BlockSpec(memory_space=pltpu.SMEM), vmem, vmem, vmem, vmem],
        out_specs=vmem,
        name="tile_product",
    )(count, table, cols, rows, blocks)


def on_device(minus_gradient, diag_blocks, hess_blocks, block_rows, block_cols, block_counts):
    pose_dev = minus_gradient.shape[1]
    high = pose_dev // LANES
    n_row = lax.axis_size("row")
    n_col = lax.axis_size("col")
    rows_own = 6 * high
    diag = diag_blocks.reshape(36, high, LANES)
    blocks = hess_blocks.reshape(36, -1)
    rows = block_rows.reshape(1, -1)
    cols = block_cols.reshape(1, -1)
    lower_part, reciprocals = factor_blocks(diag)

    def precondition(vector):
        return jnp.stack(apply_inverse(lower_part, reciprocals, vector))

    def lane_sums(left_a, right_a, left_b, right_b):
        first = jnp.sum(left_a * right_a, axis=(0, 1))
        second = jnp.sum(left_b * right_b, axis=(0, 1))
        return jnp.stack([first, second])

    def hessian(vector, sums):
        mine = jnp.concatenate([vector.reshape(rows_own, LANES), sums], axis=0)
        sent = jnp.broadcast_to(mine[None], (n_col,) + mine.shape)
        got = lax.all_to_all(sent, "col", 0, 0)
        table = got[:, :rows_own].reshape(n_col, 6, high, LANES)
        table = jnp.transpose(table, (1, 0, 2, 3)).reshape(6 * n_col * high, LANES)
        group_sums = jnp.sum(got[:, rows_own:], axis=0)
        partial = tile_product(block_counts, table, cols, rows, blocks, n_row * high)
        partial = jnp.transpose(partial.reshape(6, n_row, high, LANES), (1, 0, 2, 3))
        partial = partial.reshape(n_row, rows_own, LANES)
        spread_sums = jnp.broadcast_to(group_sums[None], (n_row,) + group_sums.shape)
        back = lax.all_to_all(jnp.concatenate([partial, spread_sums], axis=1), "row", 0, 0)
        back = jnp.sum(back, axis=0)
        own_term = jnp.sum(diag.reshape(6, 6, high, LANES) * vector[None], axis=1)
        image = back[:rows_own].reshape(6, high, LANES) + own_term
        return image, jnp.sum(back[rows_own:], axis=1)

    def total_sums(sums):
        sent = jnp.broadcast_to(sums[None], (n_col,) + sums.shape)
        sums = jnp.sum(lax.all_to_all(sent, "col", 0, 0), axis=0)
        sent = jnp.broadcast_to(sums[None], (n_row,) + sums.shape)
        sums = jnp.sum(lax.all_to_all(sent, "row", 0, 0), axis=0)
        return jnp.sum(sums, axis=1)

    residual = minus_gradient.reshape(6, high, LANES)
    update = jnp.zeros_like(residual)
    precond = precondition(residual)
    image, unused = hessian(precond, jnp.zeros((2, LANES), jnp.float32))
    for k in range(ITERS):
        sums = lane_sums(residual, precond, image, precond)
        last = k + 1 == ITERS
        if last:
            totals = total_sums(sums)
        else:
            image_pre = precondition(image)
            image_next, totals = hessian(image_pre, sums)
        rho, curv = totals[0], totals[1]
        if k == 0:
            step = rho / curv
            direction, along = precond, image
        else:
            ratio = rho / rho_before
            step = rho / (curv - ratio * rho / step)
            direction = precond + ratio * direction
            along = image + ratio * along
        update = update + step * direction
        residual = residual - step * along
        if not last:
            if k == 0:
                along_pre, along_next = image_pre, image_next
            else:
                along_pre = image_pre + ratio * along_pre
                along_next = image_next + ratio * along_next
            precond = precond - step * along_pre
            image = image - step * along_next
        rho_before = rho
    return (update.reshape(6, pose_dev), residual.reshape(6, pose_dev))


def solution(mesh):
    vectors = P(None, ("row", "col"))
    return jax.shard_map(
        on_device,
        mesh=mesh,
        in_specs=(
            vectors,
            vectors,
            P("row", "col", None, None),
            P("row", "col", None),
            P("row", "col", None),
            P("row", "col"),
        ),
        out_specs=(vectors, vectors),
        check_vma=False,
    )
```

```python
import math

import jax
import jax.numpy as jnp
from jax import lax
from jax.experimental import pallas as pl
from jax.experimental.pallas import tpu as pltpu
from jax.sharding import PartitionSpec as P

ITERS = 3
LANES = 128
SUBS = 8


def factor_blocks(blocks):
    lower_part = {}
    reciprocals = []
    for j in range(6):
        pivot_value = blocks[7 * j]
        for k in range(j):
            pivot_value = pivot_value - lower_part[j, k] * lower_part[j, k]
        reciprocal = 1.0 / jnp.sqrt(pivot_value)
        reciprocals.append(reciprocal)
        for i in range(j + 1, 6):
            entry_value = blocks[6 * i + j]
            for k in range(j):
                entry_value = entry_value - lower_part[i, k] * lower_part[j, k]
            lower_part[i, j] = entry_value * reciprocal
    return (lower_part, reciprocals)


def apply_inverse(lower_part, reciprocals, vector):
    forward = []
    for i in range(6):
        running = vector[i]
        for k in range(i):
            running = running - lower_part[i, k] * forward[k]
        forward.append(running * reciprocals[i])
    backward = [None] * 6
    for i in range(5, -1, -1):
        running = forward[i]
        for k in range(i + 1, 6):
            running = running - lower_part[k, i] * backward[k]
        backward[i] = running * reciprocals[i]
    return backward


def split_three(value):
    high = value.astype(jnp.bfloat16)
    rest = value - high.astype(jnp.float32)
    middle = rest.astype(jnp.bfloat16)
    low = (rest - middle.astype(jnp.float32)).astype(jnp.bfloat16)
    return high, middle, low


def exact_dot(left, onehot, dims):
    parts = [
        lax.dot_general(piece, onehot, (dims, ((), ())), preferred_element_type=jnp.float32)
        for piece in split_three(left)
    ]
    return parts[2] + parts[1] + parts[0]


def tile_kernel(count_ref, got_ref, cols_ref, rows_ref, blocks_ref, out_ref, *, chunk):
    n_col, high = got_ref.shape[:2]
    n_row = out_ref.shape[0]
    high_in = n_col * high
    high_out = n_row * high
    slots = cols_ref.shape[1]
    live = count_ref[0, 0]
    comp = lax.broadcasted_iota(jnp.int32, (SUBS, LANES), 0)
    sums = jnp.where(comp >= 6, sum(got_ref[c, 0] for c in range(n_col)), 0.0)
    blank = jnp.zeros((SUBS, LANES), jnp.float32)
    for r in range(n_row):
        for h in range(high):
            out_ref[r, h] = sums if h == 0 else blank

    def one_chunk(start):
        table = got_ref[...].reshape(high_in * SUBS, LANES)
        cols = cols_ref[:, pl.ds(start, chunk)]
        rows = rows_ref[:, pl.ds(start, chunk)]
        lane_ids = lax.broadcasted_iota(jnp.int32, (LANES, chunk), 0)
        low_in = jnp.where(lane_ids == cols % LANES, 1.0, 0.0).astype(jnp.bfloat16)
        spread = exact_dot(table, low_in, ((1,), (0,)))
        cols_high = jnp.broadcast_to(cols // LANES, (SUBS, chunk))
        picked = jnp.zeros((SUBS, chunk), jnp.float32)
        for t in range(high_in):
            picked = jnp.where(cols_high == t, spread[SUBS * t : SUBS * (t + 1)], picked)
        is_live = lax.broadcasted_iota(jnp.int32, (1, chunk), 1) + start < live
        terms = []
        for a in range(6):
            entries = blocks_ref[6 * a : 6 * a + 6, pl.ds(start, chunk)]
            term = jnp.sum(entries * picked[:6], axis=0, keepdims=True)
            terms.append(jnp.where(is_live, term, 0.0))
        terms.append(jnp.zeros((SUBS - 6, chunk), jnp.float32))
        terms = jnp.concatenate(terms, axis=0)
        rows_high = jnp.broadcast_to(rows // LANES, (SUBS, chunk))
        placed = jnp.concatenate(
            [jnp.where(rows_high == t, terms, 0.0) for t in range(high_out)], axis=0
        )
        low_out = jnp.where(lane_ids == rows % LANES, 1.0, 0.0).astype(jnp.bfloat16)
        added = exact_dot(placed, low_out, ((1,), (1,)))
        out_ref[...] += added.reshape(out_ref.shape)

    for turn in range(slots // chunk):
        @pl.when(turn * chunk < live)
        def _():
            one_chunk(turn * chunk)


def tile_product(count, got, cols, rows, blocks, n_row):
    chunk = math.gcd(512, cols.shape[1])
    vmem = pl.BlockSpec(memory_space=pltpu.VMEM)
    return pl.pallas_call(
        lambda *refs: tile_kernel(*refs, chunk=chunk),
        out_shape=jax.ShapeDtypeStruct((n_row,) + got.shape[1:], jnp.float32),
        in_specs=[pl.BlockSpec(memory_space=pltpu.SMEM), vmem, vmem, vmem, vmem],
        out_specs=vmem,
        name="tile_product",
    )(count, got, cols, rows, blocks)


def stage(body, inputs, out_shapes, name):
    vmem = pl.BlockSpec(memory_space=pltpu.VMEM)
    return pl.pallas_call(
        lambda *refs: body(refs[: len(inputs)], refs[len(inputs) :]),
        out_shape=[jax.ShapeDtypeStruct(s, jnp.float32) for s in out_shapes],
        in_specs=[vmem] * len(inputs),
        out_specs=[vmem] * len(out_shapes),
        name=name,
    )(*inputs)


PAIRS = [(i, j) for j in range(6) for i in range(j + 1, 6)]


def read(ref):
    return [ref[i] for i in range(ref.shape[0])]


def write(ref, values):
    for i, value in enumerate(values):
        ref[i] = value


def read_factor(ref):
    values = read(ref)
    return dict(zip(PAIRS, values[6:])), values[:6]


def axpy(left, scale, right):
    return [a + scale * b for a, b in zip(left, right)]


def lane_sums(left, right):
    total = left[0] * right[0]
    for a, b in zip(left[1:], right[1:]):
        total = total + a * b
    return jnp.sum(total, axis=0, keepdims=True)


def send(ref, vector, sums):
    copies, high = ref.shape[:2]
    blank = jnp.zeros((1, LANES), jnp.float32)
    for h in range(high):
        tail = sums if h == 0 else [blank, blank]
        tile = jnp.concatenate([v[h : h + 1] for v in vector] + tail, axis=0)
        for c in range(copies):
            ref[c, h] = tile


def receive(back_ref, diag_ref, vector):
    n_row, high = back_ref.shape[:2]
    tiles = []
    for h in range(high):
        tile = back_ref[0, h]
        for r in range(1, n_row):
            tile = tile + back_ref[r, h]
        tiles.append(tile)
    image = []
    for a in range(6):
        own = diag_ref[6 * a] * vector[0]
        for b in range(1, 6):
            own = own + diag_ref[6 * a + b] * vector[b]
        image.append(jnp.concatenate([t[a : a + 1] for t in tiles], axis=0) + own)
    rho = jnp.sum(tiles[0][6:7], axis=1, keepdims=True)
    curv = jnp.sum(tiles[0][7:8], axis=1, keepdims=True)
    return image, rho, curv


def on_device(minus_gradient, diag_blocks, hess_blocks, block_rows, block_cols, block_counts):
    pose_dev = minus_gradient.shape[1]
    high = pose_dev // LANES
    n_row = lax.axis_size("row")
    n_col = lax.axis_size("col")
    diag = diag_blocks.reshape(36, high, LANES)
    blocks = hess_blocks.reshape(36, -1)
    rows = block_rows.reshape(1, -1)
    cols = block_cols.reshape(1, -1)
    start = minus_gradient.reshape(6, high, LANES)
    vec = (6, high, LANES)
    sent_shape = (n_col, high, SUBS, LANES)
    last_shape = (n_row * n_col, 2, LANES)
    one = (1, 1)

    def exchange(sent):
        got = lax.all_to_all(sent, "col", 0, 0)
        partial = tile_product(block_counts, got, cols, rows, blocks, n_row)
        return lax.all_to_all(partial, "row", 0, 0)

    def begin(ins, outs):
        residual_ref, diag_ref = ins
        sent_ref, factor_ref, precond_ref = outs
        lower, recips = factor_blocks(diag_ref)
        write(factor_ref, recips + [lower[p] for p in PAIRS])
        precond = apply_inverse(lower, recips, read(residual_ref))
        write(precond_ref, precond)
        blank = jnp.zeros((1, LANES), jnp.float32)
        send(sent_ref, precond, [blank, blank])

    sent, factor, precond = stage(begin, [start, diag], [sent_shape, (21,) + vec[1:], vec], "begin")
    back = exchange(sent)

    def first(ins, outs):
        back_ref, diag_ref, factor_ref, residual_ref, precond_ref = ins
        sent_ref, image_ref, image_pre_ref = outs
        residual, precond = read(residual_ref), read(precond_ref)
        image, _, _ = receive(back_ref, diag_ref, precond)
        image_pre = apply_inverse(*read_factor(factor_ref), image)
        write(image_ref, image)
        write(image_pre_ref, image_pre)
        send(sent_ref, image_pre, [lane_sums(residual, precond), lane_sums(image, precond)])

    sent, image, image_pre = stage(
        first, [back, diag, factor, start, precond], [sent_shape, vec, vec], "first"
    )

    state = [start, precond, image, image_pre]
    for k in range(ITERS - 1):
        final_sums = k + 2 == ITERS
        back = exchange(sent)

        def middle(ins, outs, k=k, final_sums=final_sums):
            back_ref, diag_ref, factor_ref = ins[:3]
            residual, precond, image, image_pre = [read(r) for r in ins[3:7]]
            image_next, rho, curv = receive(back_ref, diag_ref, image_pre)
            if k == 0:
                step = rho / curv
                direction, along, along_pre, along_next = precond, image, image_pre, image_next
                update = [step * d for d in direction]
            else:
                update, direction, along, along_pre, along_next = [read(r) for r in ins[7:12]]
                rho_before, step_before = ins[12][...], ins[13][...]
                ratio = rho / rho_before
                step = rho / (curv - ratio * rho / step_before)
                direction = axpy(precond, ratio, direction)
                along = axpy(image, ratio, along)
                along_pre = axpy(image_pre, ratio, along_pre)
                along_next = axpy(image_next, ratio, along_next)
                update = axpy(update, step, direction)
            residual = axpy(residual, -step, along)
            precond = axpy(precond, -step, along_pre)
            image = axpy(image, -step, along_next)
            sums = [lane_sums(residual, precond), lane_sums(image, precond)]
            image_pre = image
            if final_sums:
                both = jnp.concatenate(sums, axis=0)
                for d in range(outs[0].shape[0]):
                    outs[0][d] = both
            else:
                image_pre = apply_inverse(*read_factor(factor_ref), image)
                send(outs[0], image_pre, sums)
            values = [residual, precond, image, image_pre, update, direction, along, along_pre, along_next]
            for ref, value in zip(outs[1:10], values):
                write(ref, value)
            outs[10][...] = rho
            outs[11][...] = step

        sent, *state = stage(
            middle,
            [back, diag, factor] + state,
            [last_shape if final_sums else sent_shape] + [vec] * 9 + [one] * 2,
            "middle",
        )

    residual, precond, image, _, update, direction, along, _, _, rho, step = state
    totals = lax.all_to_all(sent, ("row", "col"), 0, 0)

    def end(ins, outs):
        both = ins[0][0]
        for d in range(1, ins[0].shape[0]):
            both = both + ins[0][d]
        rho = jnp.sum(both[0:1], axis=1, keepdims=True)
        curv = jnp.sum(both[1:2], axis=1, keepdims=True)
        residual, precond, image, update, direction, along = [read(r) for r in ins[1:7]]
        ratio = rho / ins[7][...]
        step = rho / (curv - ratio * rho / ins[8][...])
        write(outs[0], axpy(update, step, axpy(precond, ratio, direction)))
        write(outs[1], axpy(residual, -step, axpy(image, ratio, along)))

    update, residual = stage(
        end, [totals, residual, precond, image, update, direction, along, rho, step], [vec, vec], "end"
    )
    return (update.reshape(6, pose_dev), residual.reshape(6, pose_dev))


def solution(mesh):
    vectors = P(None, ("row", "col"))
    return jax.shard_map(
        on_device,
        mesh=mesh,
        in_specs=(
            vectors,
            vectors,
            P("row", "col", None, None),
            P("row", "col", None),
            P("row", "col", None),
            P("row", "col"),
        ),
        out_specs=(vectors, vectors),
        check_vma=False,
    )
```

```python
import math

import jax
import jax.numpy as jnp
from jax import lax
from jax.experimental import pallas as pl
from jax.experimental.pallas import tpu as pltpu
from jax.sharding import PartitionSpec as P

ITERS = 3
LANES = 128
SUBS = 8


def factor_blocks(blocks):
    lower_part = {}
    reciprocals = []
    for j in range(6):
        pivot_value = blocks[7 * j]
        for k in range(j):
            pivot_value = pivot_value - lower_part[j, k] * lower_part[j, k]
        reciprocal = 1.0 / jnp.sqrt(pivot_value)
        reciprocals.append(reciprocal)
        for i in range(j + 1, 6):
            entry_value = blocks[6 * i + j]
            for k in range(j):
                entry_value = entry_value - lower_part[i, k] * lower_part[j, k]
            lower_part[i, j] = entry_value * reciprocal
    return (lower_part, reciprocals)


def apply_inverse(lower_part, reciprocals, vector):
    forward = []
    for i in range(6):
        running = vector[i]
        for k in range(i):
            running = running - lower_part[i, k] * forward[k]
        forward.append(running * reciprocals[i])
    backward = [None] * 6
    for i in range(5, -1, -1):
        running = forward[i]
        for k in range(i + 1, 6):
            running = running - lower_part[k, i] * backward[k]
        backward[i] = running * reciprocals[i]
    return backward


def split_three(value):
    high = value.astype(jnp.bfloat16)
    rest = value - high.astype(jnp.float32)
    middle = rest.astype(jnp.bfloat16)
    low = (rest - middle.astype(jnp.float32)).astype(jnp.bfloat16)
    return high, middle, low


def exact_dot(left, onehot, dims):
    parts = [
        lax.dot_general(piece, onehot, (dims, ((), ())), preferred_element_type=jnp.float32)
        for piece in split_three(left)
    ]
    return parts[2] + parts[1] + parts[0]


def tile_kernel(count_ref, cols_ref, rows_ref, blocks_ref, *refs, n_got, chunk):
    got_refs, out_refs = refs[:n_got], refs[n_got:]
    pair, high = got_refs[0].shape[:2]
    n_col = pair * n_got
    n_row = len(out_refs)
    high_in = n_col * high
    high_out = n_row * high
    slots = cols_ref.shape[1]
    live = count_ref[0, 0]
    comp = lax.broadcasted_iota(jnp.int32, (SUBS, LANES), 0)
    sums = jnp.where(comp >= 6, sum(g[c, 0] for g in got_refs for c in range(pair)), 0.0)
    blank = jnp.zeros((SUBS, LANES), jnp.float32)
    for out_ref in out_refs:
        for h in range(high):
            out_ref[h] = sums if h == 0 else blank

    def one_chunk(start):
        table = jnp.concatenate([g[...].reshape(-1, LANES) for g in got_refs], axis=0)
        cols = cols_ref[:, pl.ds(start, chunk)]
        rows = rows_ref[:, pl.ds(start, chunk)]
        lane_ids = lax.broadcasted_iota(jnp.int32, (LANES, chunk), 0)
        low_in = jnp.where(lane_ids == cols % LANES, 1.0, 0.0).astype(jnp.bfloat16)
        spread = exact_dot(table, low_in, ((1,), (0,)))
        cols_high = jnp.broadcast_to(cols // LANES, (SUBS, chunk))
        picked = jnp.zeros((SUBS, chunk), jnp.float32)
        for t in range(high_in):
            picked = jnp.where(cols_high == t, spread[SUBS * t : SUBS * (t + 1)], picked)
        is_live = lax.broadcasted_iota(jnp.int32, (1, chunk), 1) + start < live
        terms = []
        for a in range(6):
            entries = blocks_ref[6 * a : 6 * a + 6, pl.ds(start, chunk)]
            term = jnp.sum(entries * picked[:6], axis=0, keepdims=True)
            terms.append(jnp.where(is_live, term, 0.0))
        terms.append(jnp.zeros((SUBS - 6, chunk), jnp.float32))
        terms = jnp.concatenate(terms, axis=0)
        rows_high = jnp.broadcast_to(rows // LANES, (SUBS, chunk))
        placed = jnp.concatenate(
            [jnp.where(rows_high == t, terms, 0.0) for t in range(high_out)], axis=0
        )
        low_out = jnp.where(lane_ids == rows % LANES, 1.0, 0.0).astype(jnp.bfloat16)
        added = exact_dot(placed, low_out, ((1,), (1,)))
        added = added.reshape((n_row, high, SUBS, LANES))
        for r, out_ref in enumerate(out_refs):
            out_ref[...] += added[r]

    for turn in range(slots // chunk):
        @pl.when(turn * chunk < live)
        def _():
            one_chunk(turn * chunk)


def tile_product(count, got, cols, rows, blocks, n_row):
    chunk = math.gcd(512, cols.shape[1])
    vmem = pl.BlockSpec(memory_space=pltpu.VMEM)
    return pl.pallas_call(
        lambda *refs: tile_kernel(*refs, n_got=len(got), chunk=chunk),
        out_shape=[jax.ShapeDtypeStruct(got[0].shape[1:], jnp.float32)] * n_row,
        in_specs=[pl.BlockSpec(memory_space=pltpu.SMEM)] + [vmem] * (3 + len(got)),
        out_specs=[vmem] * n_row,
        name="tile_product",
    )(count, cols, rows, blocks, *got)


def swap(value, axis, distance):
    return lax.ppermute(value, axis, [(i, i ^ distance) for i in range(lax.axis_size(axis))])


def stage(body, inputs, out_shapes, name):
    vmem = pl.BlockSpec(memory_space=pltpu.VMEM)
    return pl.pallas_call(
        lambda *refs: body(refs[: len(inputs)], refs[len(inputs) :]),
        out_shape=[jax.ShapeDtypeStruct(s, jnp.float32) for s in out_shapes],
        in_specs=[vmem] * len(inputs),
        out_specs=[vmem] * len(out_shapes),
        name=name,
    )(*inputs)


PAIRS = [(i, j) for j in range(6) for i in range(j + 1, 6)]


def read(ref):
    return [ref[i] for i in range(ref.shape[0])]


def write(ref, values):
    for i, value in enumerate(values):
        ref[i] = value


def read_factor(ref):
    values = read(ref)
    return dict(zip(PAIRS, values[6:])), values[:6]


def axpy(left, scale, right):
    return [a + scale * b for a, b in zip(left, right)]


def lane_sums(left, right):
    total = left[0] * right[0]
    for a, b in zip(left[1:], right[1:]):
        total = total + a * b
    return jnp.sum(total, axis=0, keepdims=True)


def send(ref, vector, sums):
    high = ref.shape[0]
    blank = jnp.zeros((1, LANES), jnp.float32)
    for h in range(high):
        tail = sums if h == 0 else [blank, blank]
        tile = jnp.concatenate([v[h : h + 1] for v in vector] + tail, axis=0)
        ref[h] = tile


def receive(back_refs, diag_ref, vector):
    high = back_refs[0].shape[0]
    tiles = []
    for h in range(high):
        tile = back_refs[0][h]
        for back_ref in back_refs[1:]:
            tile = tile + back_ref[h]
        tiles.append(tile)
    image = []
    for a in range(6):
        own = diag_ref[6 * a] * vector[0]
        for b in range(1, 6):
            own = own + diag_ref[6 * a + b] * vector[b]
        image.append(jnp.concatenate([t[a : a + 1] for t in tiles], axis=0) + own)
    rho = jnp.sum(tiles[0][6:7], axis=1, keepdims=True)
    curv = jnp.sum(tiles[0][7:8], axis=1, keepdims=True)
    return image, rho, curv


def on_device(minus_gradient, diag_blocks, hess_blocks, block_rows, block_cols, block_counts):
    pose_dev = minus_gradient.shape[1]
    high = pose_dev // LANES
    n_row = lax.axis_size("row")
    n_col = lax.axis_size("col")
    diag = diag_blocks.reshape(36, high, LANES)
    blocks = hess_blocks.reshape(36, -1)
    rows = block_rows.reshape(1, -1)
    rows = (rows // pose_dev ^ lax.axis_index("row")) * pose_dev + rows % pose_dev
    cols = block_cols.reshape(1, -1)
    cols = (cols // pose_dev ^ lax.axis_index("col")) * pose_dev + cols % pose_dev
    start = minus_gradient.reshape(6, high, LANES)
    vec = (6, high, LANES)
    sent_shape = (high, SUBS, LANES)
    last_shape = (n_row * n_col, 2, LANES)
    one = (1, 1)

    def exchange(sent):
        pair = jnp.stack([sent, swap(sent, "col", 1)])
        got = [pair] + [swap(pair, "col", d) for d in range(2, n_col, 2)]
        parts = tile_product(block_counts, got, cols, rows, blocks, n_row)
        return [parts[0]] + [swap(parts[d], "row", d) for d in range(1, n_row)]

    def begin(ins, outs):
        residual_ref, diag_ref = ins
        sent_ref, factor_ref, precond_ref = outs
        lower, recips = factor_blocks(diag_ref)
        write(factor_ref, recips + [lower[p] for p in PAIRS])
        precond = apply_inverse(lower, recips, read(residual_ref))
        write(precond_ref, precond)
        blank = jnp.zeros((1, LANES), jnp.float32)
        send(sent_ref, precond, [blank, blank])

    sent, factor, precond = stage(begin, [start, diag], [sent_shape, (21,) + vec[1:], vec], "begin")
    back = exchange(sent)

    def first(ins, outs):
        back_refs = ins[:n_row]
        diag_ref, factor_ref, residual_ref, precond_ref = ins[n_row:]
        sent_ref, image_ref, image_pre_ref = outs
        residual, precond = read(residual_ref), read(precond_ref)
        image, _, _ = receive(back_refs, diag_ref, precond)
        image_pre = apply_inverse(*read_factor(factor_ref), image)
        write(image_ref, image)
        write(image_pre_ref, image_pre)
        send(sent_ref, image_pre, [lane_sums(residual, precond), lane_sums(image, precond)])

    sent, image, image_pre = stage(
        first, back + [diag, factor, start, precond], [sent_shape, vec, vec], "first"
    )

    state = [start, precond, image, image_pre]
    for k in range(ITERS - 1):
        final_sums = k + 2 == ITERS
        back = exchange(sent)

        def middle(ins, outs, k=k, final_sums=final_sums):
            back_refs, ins = ins[:n_row], ins[n_row:]
            diag_ref, factor_ref = ins[:2]
            residual, precond, image, image_pre = [read(r) for r in ins[2:6]]
            image_next, rho, curv = receive(back_refs, diag_ref, image_pre)
            if k == 0:
                step = rho / curv
                direction, along, along_pre, along_next = precond, image, image_pre, image_next
                update = [step * d for d in direction]
            else:
                update, direction, along, along_pre, along_next = [read(r) for r in ins[6:11]]
                rho_before, step_before = ins[11][...], ins[12][...]
                ratio = rho / rho_before
                step = rho / (curv - ratio * rho / step_before)
                direction = axpy(precond, ratio, direction)
                along = axpy(image, ratio, along)
                along_pre = axpy(image_pre, ratio, along_pre)
                along_next = axpy(image_next, ratio, along_next)
                update = axpy(update, step, direction)
            residual = axpy(residual, -step, along)
            precond = axpy(precond, -step, along_pre)
            image = axpy(image, -step, along_next)
            sums = [lane_sums(residual, precond), lane_sums(image, precond)]
            image_pre = image
            if final_sums:
                both = jnp.concatenate(sums, axis=0)
                for d in range(outs[0].shape[0]):
                    outs[0][d] = both
            else:
                image_pre = apply_inverse(*read_factor(factor_ref), image)
                send(outs[0], image_pre, sums)
            values = [residual, precond, image, image_pre, update, direction, along, along_pre, along_next]
            for ref, value in zip(outs[1:10], values):
                write(ref, value)
            outs[10][...] = rho
            outs[11][...] = step

        sent, *state = stage(
            middle,
            back + [diag, factor] + state,
            [last_shape if final_sums else sent_shape] + [vec] * 9 + [one] * 2,
            "middle",
        )

    residual, precond, image, _, update, direction, along, _, _, rho, step = state
    totals = lax.all_to_all(sent, ("row", "col"), 0, 0)

    def end(ins, outs):
        both = ins[0][0]
        for d in range(1, ins[0].shape[0]):
            both = both + ins[0][d]
        rho = jnp.sum(both[0:1], axis=1, keepdims=True)
        curv = jnp.sum(both[1:2], axis=1, keepdims=True)
        residual, precond, image, update, direction, along = [read(r) for r in ins[1:7]]
        ratio = rho / ins[7][...]
        step = rho / (curv - ratio * rho / ins[8][...])
        write(outs[0], axpy(update, step, axpy(precond, ratio, direction)))
        write(outs[1], axpy(residual, -step, axpy(image, ratio, along)))

    update, residual = stage(
        end, [totals, residual, precond, image, update, direction, along, rho, step], [vec, vec], "end"
    )
    return (update.reshape(6, pose_dev), residual.reshape(6, pose_dev))


def solution(mesh):
    vectors = P(None, ("row", "col"))
    return jax.shard_map(
        on_device,
        mesh=mesh,
        in_specs=(
            vectors,
            vectors,
            P("row", "col", None, None),
            P("row", "col", None),
            P("row", "col", None),
            P("row", "col"),
        ),
        out_specs=(vectors, vectors),
        check_vma=False,
    )
```

```python
import math

import jax
import jax.numpy as jnp
from jax import lax
from jax.experimental import pallas as pl
from jax.experimental.pallas import tpu as pltpu
from jax.sharding import PartitionSpec as P

ITERS = 3
LANES = 128
SUBS = 8


def factor_blocks(blocks):
    lower_part = {}
    reciprocals = []
    for j in range(6):
        pivot_value = blocks[7 * j]
        for k in range(j):
            pivot_value = pivot_value - lower_part[j, k] * lower_part[j, k]
        reciprocal = 1.0 / jnp.sqrt(pivot_value)
        reciprocals.append(reciprocal)
        for i in range(j + 1, 6):
            entry_value = blocks[6 * i + j]
            for k in range(j):
                entry_value = entry_value - lower_part[i, k] * lower_part[j, k]
            lower_part[i, j] = entry_value * reciprocal
    return (lower_part, reciprocals)


def apply_inverse(lower_part, reciprocals, vector):
    forward = []
    for i in range(6):
        running = vector[i]
        for k in range(i):
            running = running - lower_part[i, k] * forward[k]
        forward.append(running * reciprocals[i])
    backward = [None] * 6
    for i in range(5, -1, -1):
        running = forward[i]
        for k in range(i + 1, 6):
            running = running - lower_part[k, i] * backward[k]
        backward[i] = running * reciprocals[i]
    return backward


def split_three(value):
    high = value.astype(jnp.bfloat16)
    rest = value - high.astype(jnp.float32)
    middle = rest.astype(jnp.bfloat16)
    low = (rest - middle.astype(jnp.float32)).astype(jnp.bfloat16)
    return high, middle, low


def exact_dot(left, onehot, dims):
    parts = [
        lax.dot_general(piece, onehot, (dims, ((), ())), preferred_element_type=jnp.float32)
        for piece in split_three(left)
    ]
    return parts[2] + parts[1] + parts[0]


def tile_kernel(count_ref, cols_ref, rows_ref, blocks_ref, *refs, n_got, chunk):
    got_refs, out_refs = refs[:n_got], refs[n_got:]
    pair, high = got_refs[0].shape[:2]
    n_col = pair * n_got
    n_row = len(out_refs)
    high_in = n_col * high
    high_out = n_row * high
    slots = cols_ref.shape[1]
    live = count_ref[0, 0]
    comp = lax.broadcasted_iota(jnp.int32, (SUBS, LANES), 0)
    sums = jnp.where(comp >= 6, sum(g[c, 0] for g in got_refs for c in range(pair)), 0.0)
    blank = jnp.zeros((SUBS, LANES), jnp.float32)
    for out_ref in out_refs:
        for h in range(high):
            out_ref[h] = sums if h == 0 else blank

    def one_chunk(start):
        table = jnp.concatenate([g[...].reshape(-1, LANES) for g in got_refs], axis=0)
        cols = cols_ref[:, pl.ds(start, chunk)]
        rows = rows_ref[:, pl.ds(start, chunk)]
        lane_ids = lax.broadcasted_iota(jnp.int32, (LANES, chunk), 0)
        low_in = jnp.where(lane_ids == cols % LANES, 1.0, 0.0).astype(jnp.bfloat16)
        spread = exact_dot(table, low_in, ((1,), (0,)))
        cols_high = jnp.broadcast_to(cols // LANES, (SUBS, chunk))
        picked = jnp.zeros((SUBS, chunk), jnp.float32)
        for t in range(high_in):
            picked = jnp.where(cols_high == t, spread[SUBS * t : SUBS * (t + 1)], picked)
        is_live = lax.broadcasted_iota(jnp.int32, (1, chunk), 1) + start < live
        terms = []
        for a in range(6):
            entries = blocks_ref[0, 0, 6 * a : 6 * a + 6, pl.ds(start, chunk)]
            term = jnp.sum(entries * picked[:6], axis=0, keepdims=True)
            terms.append(jnp.where(is_live, term, 0.0))
        terms.append(jnp.zeros((SUBS - 6, chunk), jnp.float32))
        terms = jnp.concatenate(terms, axis=0)
        rows_high = jnp.broadcast_to(rows // LANES, (SUBS, chunk))
        placed = jnp.concatenate(
            [jnp.where(rows_high == t, terms, 0.0) for t in range(high_out)], axis=0
        )
        low_out = jnp.where(lane_ids == rows % LANES, 1.0, 0.0).astype(jnp.bfloat16)
        added = exact_dot(placed, low_out, ((1,), (1,)))
        added = added.reshape((n_row, high, SUBS, LANES))
        for r, out_ref in enumerate(out_refs):
            out_ref[...] += added[r]

    for turn in range(slots // chunk):
        @pl.when(turn * chunk < live)
        def _():
            one_chunk(turn * chunk)


def tile_product(count, got, cols, rows, blocks, n_row):
    chunk = math.gcd(512, cols.shape[1])
    vmem = pl.BlockSpec(memory_space=pltpu.VMEM)
    return pl.pallas_call(
        lambda *refs: tile_kernel(*refs, n_got=len(got), chunk=chunk),
        out_shape=[jax.ShapeDtypeStruct(got[0].shape[1:], jnp.float32)] * n_row,
        in_specs=[pl.BlockSpec(memory_space=pltpu.SMEM)] + [vmem] * (3 + len(got)),
        out_specs=[vmem] * n_row,
        name="tile_product",
    )(count, cols, rows, blocks, *got)


def swap(value, axis, distance):
    return lax.ppermute(value, axis, [(i, i ^ distance) for i in range(lax.axis_size(axis))])


def stage(body, inputs, out_shapes, name):
    vmem = pl.BlockSpec(memory_space=pltpu.VMEM)
    return pl.pallas_call(
        lambda *refs: body(refs[: len(inputs)], refs[len(inputs) :]),
        out_shape=[jax.ShapeDtypeStruct(s, jnp.float32) for s in out_shapes],
        in_specs=[vmem] * len(inputs),
        out_specs=[vmem] * len(out_shapes),
        name=name,
    )(*inputs)


PAIRS = [(i, j) for j in range(6) for i in range(j + 1, 6)]


def read(ref):
    return [ref[i] for i in range(ref.shape[0])]


def write(ref, values):
    for i, value in enumerate(values):
        ref[i] = value


def read_wide(ref):
    tiles = [ref[:, h : h + LANES] for h in range(0, ref.shape[1], LANES)]
    return [
        jnp.concatenate([t[i : i + 1] for t in tiles], axis=0) for i in range(ref.shape[0])
    ]


def write_wide(ref, values):
    for h in range(values[0].shape[0]):
        tile = jnp.concatenate([v[h : h + 1] for v in values], axis=0)
        ref[:, LANES * h : LANES * (h + 1)] = tile


def read_factor(ref):
    values = read(ref)
    return dict(zip(PAIRS, values[6:])), values[:6]


def axpy(left, scale, right):
    return [a + scale * b for a, b in zip(left, right)]


def lane_sums(left, right):
    total = left[0] * right[0]
    for a, b in zip(left[1:], right[1:]):
        total = total + a * b
    return jnp.sum(total, axis=0, keepdims=True)


def send(ref, vector, sums):
    high = ref.shape[0]
    blank = jnp.zeros((1, LANES), jnp.float32)
    for h in range(high):
        tail = sums if h == 0 else [blank, blank]
        tile = jnp.concatenate([v[h : h + 1] for v in vector] + tail, axis=0)
        ref[h] = tile


def receive(back_refs, diag_ref, vector):
    high = back_refs[0].shape[0]
    tiles = []
    for h in range(high):
        tile = back_refs[0][h]
        for back_ref in back_refs[1:]:
            tile = tile + back_ref[h]
        tiles.append(tile)
    image = []
    for a in range(6):
        own = diag_ref[6 * a] * vector[0]
        for b in range(1, 6):
            own = own + diag_ref[6 * a + b] * vector[b]
        image.append(jnp.concatenate([t[a : a + 1] for t in tiles], axis=0) + own)
    rho = jnp.sum(tiles[0][6:7], axis=1, keepdims=True)
    curv = jnp.sum(tiles[0][7:8], axis=1, keepdims=True)
    return image, rho, curv


def on_device(minus_gradient, diag_blocks, hess_blocks, block_rows, block_cols, block_counts):
    pose_dev = minus_gradient.shape[1]
    high = pose_dev // LANES
    n_row = lax.axis_size("row")
    n_col = lax.axis_size("col")
    rows = block_rows.reshape(1, -1)
    rows = (rows // pose_dev ^ lax.axis_index("row")) * pose_dev + rows % pose_dev
    cols = block_cols.reshape(1, -1)
    cols = (cols // pose_dev ^ lax.axis_index("col")) * pose_dev + cols % pose_dev
    vec = (6, high, LANES)
    sent_shape = (high, SUBS, LANES)
    last_shape = (n_row * n_col, 2, LANES)
    one = (1, 1)

    def exchange(sent):
        pair = jnp.stack([sent, swap(sent, "col", 1)])
        got = [pair] + [swap(pair, "col", d) for d in range(2, n_col, 2)]
        parts = tile_product(block_counts, got, cols, rows, hess_blocks, n_row)
        return [parts[0]] + [swap(parts[d], "row", d) for d in range(1, n_row)]

    def begin(ins, outs):
        sent_ref, factor_ref, precond_ref, residual_ref, diag_ref = outs
        residual, diag = read_wide(ins[0]), read_wide(ins[1])
        write(residual_ref, residual)
        write(diag_ref, diag)
        lower, recips = factor_blocks(diag)
        write(factor_ref, recips + [lower[p] for p in PAIRS])
        precond = apply_inverse(lower, recips, residual)
        write(precond_ref, precond)
        blank = jnp.zeros((1, LANES), jnp.float32)
        send(sent_ref, precond, [blank, blank])

    sent, factor, precond, start, diag = stage(
        begin,
        [minus_gradient, diag_blocks],
        [sent_shape, (21,) + vec[1:], vec, vec, (36,) + vec[1:]],
        "begin",
    )
    back = exchange(sent)

    def first(ins, outs):
        back_refs = ins[:n_row]
        diag_ref, factor_ref, residual_ref, precond_ref = ins[n_row:]
        sent_ref, image_ref, image_pre_ref = outs
        residual, precond = read(residual_ref), read(precond_ref)
        image, _, _ = receive(back_refs, diag_ref, precond)
        image_pre = apply_inverse(*read_factor(factor_ref), image)
        write(image_ref, image)
        write(image_pre_ref, image_pre)
        send(sent_ref, image_pre, [lane_sums(residual, precond), lane_sums(image, precond)])

    sent, image, image_pre = stage(
        first, back + [diag, factor, start, precond], [sent_shape, vec, vec], "first"
    )

    state = [start, precond, image, image_pre]
    for k in range(ITERS - 1):
        final_sums = k + 2 == ITERS
        back = exchange(sent)

        def middle(ins, outs, k=k, final_sums=final_sums):
            back_refs, ins = ins[:n_row], ins[n_row:]
            diag_ref, factor_ref = ins[:2]
            residual, precond, image, image_pre = [read(r) for r in ins[2:6]]
            image_next, rho, curv = receive(back_refs, diag_ref, image_pre)
            if k == 0:
                step = rho / curv
                direction, along, along_pre, along_next = precond, image, image_pre, image_next
                update = [step * d for d in direction]
            else:
                update, direction, along, along_pre, along_next = [read(r) for r in ins[6:11]]
                rho_before, step_before = ins[11][...], ins[12][...]
                ratio = rho / rho_before
                step = rho / (curv - ratio * rho / step_before)
                direction = axpy(precond, ratio, direction)
                along = axpy(image, ratio, along)
                along_pre = axpy(image_pre, ratio, along_pre)
                along_next = axpy(image_next, ratio, along_next)
                update = axpy(update, step, direction)
            residual = axpy(residual, -step, along)
            precond = axpy(precond, -step, along_pre)
            image = axpy(image, -step, along_next)
            sums = [lane_sums(residual, precond), lane_sums(image, precond)]
            image_pre = image
            if final_sums:
                both = jnp.concatenate(sums, axis=0)
                for d in range(outs[0].shape[0]):
                    outs[0][d] = both
            else:
                image_pre = apply_inverse(*read_factor(factor_ref), image)
                send(outs[0], image_pre, sums)
            values = [residual, precond, image, image_pre, update, direction, along, along_pre, along_next]
            for ref, value in zip(outs[1:10], values):
                write(ref, value)
            outs[10][...] = rho
            outs[11][...] = step

        sent, *state = stage(
            middle,
            back + [diag, factor] + state,
            [last_shape if final_sums else sent_shape] + [vec] * 9 + [one] * 2,
            "middle",
        )

    residual, precond, image, _, update, direction, along, _, _, rho, step = state
    totals = lax.all_to_all(sent, ("row", "col"), 0, 0)

    def end(ins, outs):
        both = ins[0][0]
        for d in range(1, ins[0].shape[0]):
            both = both + ins[0][d]
        rho = jnp.sum(both[0:1], axis=1, keepdims=True)
        curv = jnp.sum(both[1:2], axis=1, keepdims=True)
        residual, precond, image, update, direction, along = [read(r) for r in ins[1:7]]
        ratio = rho / ins[7][...]
        step = rho / (curv - ratio * rho / ins[8][...])
        write_wide(outs[0], axpy(update, step, axpy(precond, ratio, direction)))
        write_wide(outs[1], axpy(residual, -step, axpy(image, ratio, along)))

    return tuple(
        stage(
            end,
            [totals, residual, precond, image, update, direction, along, rho, step],
            [minus_gradient.shape] * 2,
            "end",
        )
    )


def solution(mesh):
    vectors = P(None, ("row", "col"))
    return jax.shard_map(
        on_device,
        mesh=mesh,
        in_specs=(
            vectors,
            vectors,
            P("row", "col", None, None),
            P("row", "col", None),
            P("row", "col", None),
            P("row", "col"),
        ),
        out_specs=(vectors, vectors),
        check_vma=False,
    )
```
